32 devices in a mesh: row: 8 (over z, x), col: 2 (over y), rep: 2 (over core).
Axes of the slice: x: 2, y: 2, z: 4, core: 2. Of those that a mesh axis runs over, the one named last changes fastest.
Arguments:
- matrix: float32 [16384, 16384], P('row', 'col'), may hold values from -0.125 to 0.125
- vectors: float32 [64, 16384], P('rep', 'row'), may hold values from -0.3 to 0.3
Outputs:
- result: float32 [64, 16384], P('rep', 'row')
The draws below stay inside these ranges and needn't reach their ends.
All inputs are finite; a program needn't handle non-finite values.
Results may differ from the reference program's by a relative error of at most 0.00011.
Values sent between devices are 32-bit elements; how exact they have to be, the bound alone decides.
A program may use at most 128 MiB of HBM per device.

```python
import jax
import jax.numpy as jnp
from jax import lax

N = 16384
COLS = 64
TERMS = 6
STEPS = 1


def block_scale(rng, dims, split, smallest, largest):
    factor_of = 1.0
    for position, blocks in split:
        steps = jax.random.uniform(jax.random.fold_in(jax.random.fold_in(rng, 6), position), (blocks,), jnp.float32, smallest / len(split), largest / len(split))
        factor_of = factor_of * jnp.repeat(jnp.exp(steps), dims[position] // blocks).reshape((-1,) + (1,) * (len(dims) - 1 - position))
    return factor_of


def gaussian(stream_key, shape, deviation, limit, pieces=(), dtype=jnp.bfloat16):
    factor_of = block_scale(stream_key, shape, pieces, -0.22, 0.18) if pieces else 1.0
    entries = jax.random.normal(stream_key, shape, jnp.float32) * deviation * factor_of
    return jnp.minimum(jnp.maximum(entries, -limit), limit).astype(dtype)


def setup_inputs(seed: int = 0) -> dict:
    key_list = jax.random.split(jax.random.key(seed), 3)
    matrix = gaussian(key_list[0], (N, N), (N // 7) ** -0.5, 0.125, ((0, 8), (1, 2)), jnp.float32)
    vectors = gaussian(key_list[1], (COLS, N), 0.05, 0.3, ((0, 2), (1, 8)), jnp.float32)
    return {"matrix": matrix, "vectors": vectors}


def reference(matrix, vectors):
    current = vectors
    for section in range(STEPS):
        summand = current
        running = current
        for degree in range(1, TERMS + 1):
            product = lax.dot_general(summand, matrix, (((1,), (1,)), ((), ())), precision=lax.Precision.HIGHEST, preferred_element_type=jnp.float32)
            summand = product / float(degree * STEPS)
            running = running + summand
        current = running
    return current
```

```python
import functools

import jax
import jax.numpy as jnp
from jax import lax
from jax.experimental import pallas as pl
from jax.experimental.pallas import tpu as pltpu
from jax.sharding import PartitionSpec as P

TERMS = 6
STEPS = 1
MESH = pl.DeviceIdType.MESH
TILE = 256
SLOTS = 4
LAG = 5
SUM_AT = 3


def kernel(rows, cols, groups, *refs):
    tiles = refs[0].shape[0] // TILE
    part = refs[1].shape[0]
    sums = [pltpu.ACC(n % 2)((part, TILE), jnp.float32) for n in range(tiles)]
    pl.run_scoped(lambda *sums: body(rows, cols, groups, sums, *refs), *sums)


def body(
    rows, cols, groups, sums, m_ref, v_ref, out_ref,
    high, low, stage, xbuf, sbuf, acc, drecv, ybuf, run, fin, frecv,
    stage_sem, init_send, init_recv, x_recv, line_send, pair_send,
    d_send, d_recv, y_send, y_recv, f_send, f_recv,
):
    fanout = rows // cols
    size = m_ref.shape[0]
    part = v_ref.shape[0]
    half = size // 2
    chunks = half // TILE
    tiles = size // TILE
    lines = rows // 2
    depth = fanout // 2
    total = fanout * chunks
    last = TERMS - 1

    r, c, p = lax.axis_index("row"), lax.axis_index("col"), lax.axis_index("rep")
    z, x = r // 2, r % 2
    first_line = c * depth
    owner = r // fanout
    own = owner == c
    helper = (owner + 1) % cols
    aid = (helper == c) & (depth > 1)
    mine = r % fanout

    barrier = pltpu.get_barrier_semaphore()

    def greet(**where):
        pl.semaphore_signal(barrier, inc=1, device_id=where, device_id_type=MESH)

    greet(rep=1 - p)
    greet(row=z * 2 + 1 - x)
    for other in range(1, lines * cols):
        greet(row=(z + other // cols) % lines * 2 + x, col=(c + other % cols) % cols)

    def chunk_of(step):
        count = total // 2
        lag = min(LAG, count)
        mixed = step - lag
        alternate = jnp.where(mixed % 2 == 0, count + mixed // 2, lag + mixed // 2)
        place = jnp.where(step < lag, step, jnp.where(step < 2 * count - lag, alternate, step))
        other, place = place // count, place % count
        near = jnp.where(own, place // chunks, place % depth)
        line = jnp.where(z > first_line, depth - 1 - near, near)
        lane = jnp.where(other == 0, x, 1 - x)
        return line, lane, line * 2 + lane, jnp.where(own, place % chunks, place // depth)

    def load(step):
        _, _, j, k = chunk_of(step)
        start = pl.multiple_of(j * size + p * half + k * TILE, TILE)
        return pltpu.make_async_copy(
            m_ref.at[:, pl.ds(start, TILE)], stage.at[step % SLOTS], stage_sem.at[step % SLOTS]
        )

    for step in range(min(SLOTS, total)):
        load(step).start()

    for total_ref in sums:
        pltpu.matmul_pop(total_ref)

    pl.semaphore_wait(barrier, lines * cols + 1)

    def remote(source, target, send, recv, **where):
        return pltpu.make_async_remote_copy(
            src_ref=source, dst_ref=target, send_sem=send, recv_sem=recv,
            device_id=where, device_id_type=MESH,
        )

    def relay(s, h, j, k):
        ref = xbuf.at[s, h, j, k]
        return remote(ref, ref, pair_send.at[h, j, k], x_recv.at[s % 2, h, j, k], row=z * 2 + 1 - x)

    def routes(s, h, k):
        first = owner * depth
        top = first + depth - 1
        source, target, recv = sbuf.at[s, h, k], xbuf.at[s, h, mine, k], x_recv.at[s % 2, h, mine, k]
        for t in range(lines):
            inside = (t >= first) & (t <= top)
            direct = inside | (jnp.where(t > top, top, first) == z)
            needed = (t != z) & ((own & direct) | (aid & jnp.logical_not(direct)))
            yield needed, remote(source, target, line_send.at[h, t, k], recv, row=t * 2 + x, col=owner)
        yield own, remote(source, target, pair_send.at[h, mine, k], recv, row=z * 2 + 1 - x)

    def spread(s, h, k, again):
        for needed, copy in routes(s, h, k):
            @pl.when(needed)
            def _(copy=copy):
                if again:
                    copy.wait_send()
                copy.start()

    @pl.when(own | aid)
    def _():
        def given(k):
            start = pl.multiple_of((1 - p) * half + k * TILE, TILE)
            return remote(
                v_ref.at[:, pl.ds(start, TILE)], sbuf.at[0, p, k], init_send.at[k], init_recv.at[k], rep=1 - p,
            )

        for k in range(chunks):
            given(k).start()
        for k in range(chunks):
            start = pl.multiple_of(p * half + k * TILE, TILE)
            sbuf[0, p, k] = v_ref[:, pl.ds(start, TILE)]
        for k in range(chunks):
            given(k).wait()
            spread(0, 0, k, False)
        for h in range(1, groups):
            for k in range(chunks):
                spread(0, h, k, False)

    @pl.when(own)
    def _():
        for h in range(groups):
            for k in range(chunks):
                run[h, k] = sbuf[0, h, k]
                xbuf[0, h, mine, k] = sbuf[0, h, k]

    @pl.when(jnp.logical_not(own))
    def _():
        run[...] = jnp.zeros_like(run)

    def prepare(step, index):
        load(step).wait()
        for n in range(tiles):
            block = stage[step % SLOTS, n * TILE:(n + 1) * TILE, :]
            top = block.astype(jnp.bfloat16)
            rest = (block - top.astype(jnp.float32)).astype(jnp.bfloat16)
            high[index, n] = top.T
            low[index, n] = rest.T

        @pl.when(step + SLOTS < total)
        def _():
            load(step + SLOTS).start()

    def gather(s, h, step, again):
        _, lane, j, k = chunk_of(step)

        @pl.when(r != c * fanout + j)
        def _():
            copy = relay(s, h, j, k)
            copy.wait_recv()

            @pl.when(lane == x)
            def _():
                if again:
                    copy.wait_send()
                copy.start()

    def multiply(s, h, step):
        _, _, j, k = chunk_of(step)
        index = j * chunks + k
        value = xbuf[s, h, j, k]
        top = value.astype(jnp.bfloat16)
        rest = (value - top.astype(jnp.float32)).astype(jnp.bfloat16)
        for n in range(tiles):
            pltpu.matmul_push_rhs(high[index, n], staging_register=0, mxu_index=n % 2)
            pltpu.matmul_acc_lhs(sums[n], top, load_staged_rhs=0)
            pltpu.matmul_acc_lhs(sums[n], rest)
            pltpu.matmul_push_rhs(low[index, n], staging_register=1, mxu_index=n % 2)
            pltpu.matmul_acc_lhs(sums[n], top, load_staged_rhs=1)

    def swap(s, h, k):
        return remote(
            acc.at[h, (1 - p) * chunks + k], drecv.at[s, h, k],
            d_send.at[h, k], d_recv.at[s % 2, h, k], rep=1 - p,
        )

    def close(s, h):
        for n in range(tiles):
            acc[h, n] = pltpu.matmul_pop(sums[n])
        for k in range(chunks):
            swap(s, h, k).start()

    def to_column(s, h, k, target):
        ref = ybuf.at[s, h, c, k]
        return remote(ref, ref, y_send.at[target, h, k], y_recv.at[s % 2, c, h, k], col=target)

    def from_column(s, h, k, source):
        ref = ybuf.at[s, h, source, k]
        return remote(ref, ref, y_send.at[source, h, k], y_recv.at[s % 2, source, h, k], col=source)

    def column_sum(s, h, k):
        for offset in range(1, cols):
            from_column(s, h, k, (c + offset) % cols).wait_recv()
        value = ybuf[s, h, 0, k]
        for source in range(1, cols):
            value = value + ybuf[s, h, source, k]
        return value

    def scaled(s, h, k):
        swap(s, h, k).wait_recv()
        degree = jnp.asarray((s + 1) * STEPS, jnp.int32).astype(jnp.float32)
        return (acc[h, p * chunks + k] + drecv[s, h, k]) / degree

    def to_makers(s, h, k, visit):
        for target, there in ((owner, True), (helper, depth > 1)):
            if there:
                @pl.when(c != target)
                def _(target=target):
                    visit(to_column(s, h, k, target))

    def add_up(s, h):
        for k in range(chunks):
            ybuf[s, h, c, k] = scaled(s, h, k)

            @pl.when(s > 0)
            def _(k=k):
                to_makers(s, h, k, lambda copy: copy.wait_send())

            to_makers(s, h, k, lambda copy: copy.start())

        @pl.when(aid)
        def _():
            for k in range(chunks):
                sbuf[s + 1, h, k] = column_sum(s, h, k)
                spread(s + 1, h, k, True)

    def send_out(s, h, k):
        @pl.when(own)
        def _():
            value = column_sum(s, h, k)
            sbuf[s + 1, h, k] = value
            spread(s + 1, h, k, True)
            xbuf[s + 1, h, mine, k] = value
            run[h, k] = run[h, k] + value

        swap(s, h, k).wait_send()

    def add_up_last(h):
        for k in range(chunks):
            ybuf[last, h, c, k] = scaled(last, h, k) + run[h, k]

            to_makers(last, h, k, lambda copy: copy.wait_send())
            for offset in range(1, cols):
                to_column(last, h, k, (c + offset) % cols).start()

    def give(k):
        return remote(fin.at[k], frecv.at[k], f_send.at[k], f_recv.at[k], rep=1 - p)

    def finish(h, k):
        value = column_sum(last, h, k)

        @pl.when(p == h)
        def _():
            start = pl.multiple_of(p * half + k * TILE, TILE)
            out_ref[:, pl.ds(start, TILE)] = value

        @pl.when(p != h)
        def _():
            fin[k] = value
            give(k).start()

        swap(last, h, k).wait_send()

    sum_at = SUM_AT * total // 16

    def opening(step, carry):
        _, _, j, k = chunk_of(step)
        prepare(step, j * chunks + k)
        gather(0, 0, step, False)
        multiply(0, 0, step)
        for h in range(1, groups):
            gather(0, h, step, False)
        return carry

    lax.fori_loop(0, total, opening, 0)
    close(0, 0)

    def loop(s, h, again, begin, each):
        def run_step(step, carry):
            if again:
                gather(s, h, step, True)
            multiply(s, h, step)

            @pl.when(step == sum_at)
            def _():
                begin()

            return carry

        lax.fori_loop(0, total, run_step, 0)
        close(s, h)
        for k in range(chunks):
            each(k)

    def behind(s, h):
        return functools.partial(add_up, s, h), functools.partial(send_out, s, h)

    for h in range(1, groups):
        loop(0, h, False, *behind(0, h - 1))

    def middle(s, carry):
        loop(s, 0, True, *behind(s - 1, groups - 1))
        for h in range(1, groups):
            loop(s, h, True, *behind(s, h - 1))
        return carry

    lax.fori_loop(1, last, middle, 0)
    loop(last, 0, True, *behind(last - 1, groups - 1))
    for h in range(1, groups):
        loop(last, h, True, functools.partial(add_up_last, h - 1), functools.partial(finish, h - 1))
    add_up_last(groups - 1)
    for k in range(chunks):
        finish(groups - 1, k)

    for k in range(chunks):
        give(k).wait()
        start = pl.multiple_of((1 - p) * half + k * TILE, TILE)
        out_ref[:, pl.ds(start, TILE)] = frecv[k]
        for h in range(groups):
            for offset in range(1, cols):
                to_column(last, h, k, (c + offset) % cols).wait_send()

    def drain(step, carry):
        _, lane, j, k = chunk_of(step)

        @pl.when(lane == x)
        def _():
            for h in range(groups):
                relay(last, h, j, k).wait_send()

        return carry

    lax.fori_loop(0, total, drain, 0)
    for h in range(groups):
        for k in range(chunks):
            for needed, copy in list(routes(last, h, k))[:-1]:
                @pl.when(needed)
                def _(copy=copy):
                    copy.wait_send()


def solution(mesh):
    rows, cols, groups = (mesh.shape[axis] for axis in ("row", "col", "rep"))

    def local(matrix, vectors):
        size, width = matrix.shape
        part = vectors.shape[0]
        fanout = rows // cols
        chunks = size // 2 // TILE
        tiles = size // TILE
        piece = (part, TILE)
        dma = pltpu.SemaphoreType.DMA
        return pl.pallas_call(
            functools.partial(kernel, rows, cols, groups),
            out_shape=jax.ShapeDtypeStruct(vectors.shape, jnp.float32),
            in_specs=[pl.BlockSpec(memory_space=pltpu.HBM), pl.BlockSpec(memory_space=pltpu.VMEM)],
            out_specs=pl.BlockSpec(memory_space=pltpu.VMEM),
            scratch_shapes=[
                pltpu.VMEM((fanout * chunks, tiles, TILE, TILE), jnp.bfloat16),
                pltpu.VMEM((fanout * chunks, tiles, TILE, TILE), jnp.bfloat16),
                pltpu.VMEM((SLOTS, size, TILE), jnp.float32),
                pltpu.VMEM((TERMS, groups, fanout, chunks) + piece, jnp.float32),
                pltpu.VMEM((TERMS, groups, chunks) + piece, jnp.float32),
                pltpu.VMEM((groups, tiles) + piece, jnp.float32),
                pltpu.VMEM((TERMS, groups, chunks) + piece, jnp.float32),
                pltpu.VMEM((TERMS, groups, cols, chunks) + piece, jnp.float32),
                pltpu.VMEM((groups, chunks) + piece, jnp.float32),
                pltpu.VMEM((chunks,) + piece, jnp.float32),
                pltpu.VMEM((chunks,) + piece, jnp.float32),
                dma((SLOTS,)),
                dma((chunks,)),
                dma((chunks,)),
                dma((2, groups, fanout, chunks)),
                dma((groups, rows // 2, chunks)),
                dma((groups, fanout, chunks)),
                dma((groups, chunks)),
                dma((2, groups, chunks)),
                dma((cols, groups, chunks)),
                dma((2, cols, groups, chunks)),
                dma((chunks,)),
                dma((chunks,)),
            ],
            compiler_params=pltpu.CompilerParams(
                collective_id=0, has_side_effects=True, vmem_limit_bytes=63 * 1024 * 1024
            ),
        )(matrix, vectors)

    return jax.shard_map(
        local, mesh=mesh, in_specs=(P("row", "col"), P("rep", "row")), out_specs=P("rep", "row"), check_vma=False
    )
```

```python
import functools

import jax
import jax.numpy as jnp
from jax import lax
from jax.experimental import pallas as pl
from jax.experimental.pallas import tpu as pltpu
from jax.sharding import PartitionSpec as P

TERMS = 6
STEPS = 1
MESH = pl.DeviceIdType.MESH
TILE = 256
SLOTS = 4
LAG = 5
SUM_AT = 3
HELP_AT = 6
AHEAD = 1


def kernel(rows, cols, groups, *refs):
    tiles = refs[0].shape[0] // TILE
    part = refs[1].shape[0]
    sums = [pltpu.ACC(n % 2)((part, TILE), jnp.float32) for n in range(tiles)]
    pl.run_scoped(lambda *sums: body(rows, cols, groups, sums, *refs), *sums)


def body(
    rows, cols, groups, sums, m_ref, v_ref, out_ref,
    high, low, stage, xbuf, sbuf, acc, drecv, ybuf, run, fin, frecv,
    stage_sem, init_send, init_recv, x_recv, line_send, pair_send,
    d_send, d_recv, y_send, y_recv, f_send, f_recv,
):
    fanout = rows // cols
    size = m_ref.shape[0]
    part = v_ref.shape[0]
    half = size // 2
    chunks = half // TILE
    tiles = size // TILE
    lines = rows // 2
    depth = fanout // 2
    total = fanout * chunks
    last = TERMS - 1

    r, c, p = lax.axis_index("row"), lax.axis_index("col"), lax.axis_index("rep")
    z, x = r // 2, r % 2
    first_line = c * depth
    owner = r // fanout
    own = owner == c
    helper = (owner + 1) % cols
    aid = (helper == c) & (depth > 1)
    mine = r % fanout

    barrier = pltpu.get_barrier_semaphore()

    def greet(**where):
        pl.semaphore_signal(barrier, inc=1, device_id=where, device_id_type=MESH)

    greet(rep=1 - p)
    greet(row=z * 2 + 1 - x)
    for other in range(1, lines * cols):
        greet(row=(z + other // cols) % lines * 2 + x, col=(c + other % cols) % cols)

    def chunk_of(step):
        count = total // 2
        lag = min(LAG, count)
        mixed = step - lag
        alternate = jnp.where(mixed % 2 == 0, count + mixed // 2, lag + mixed // 2)
        place = jnp.where(step < lag, step, jnp.where(step < 2 * count - lag, alternate, step))
        return block_of(place // count, place % count)

    def block_of(other, place):
        near = jnp.where(own, place // chunks, place % depth)
        line = jnp.where(z > first_line, depth - 1 - near, near)
        lane = jnp.where(other == 0, x, 1 - x)
        return line, lane, line * 2 + lane, jnp.where(own, place % chunks, place // depth)

    middle_step = total // 2

    def load(turn):
        _, _, j, k = chunk_of((turn + middle_step) % total)
        start = pl.multiple_of(j * size + p * half + k * TILE, TILE)
        return pltpu.make_async_copy(
            m_ref.at[:, pl.ds(start, TILE)], stage.at[turn % SLOTS], stage_sem.at[turn % SLOTS]
        )

    for step in range(min(SLOTS, total)):
        load(step).start()

    for total_ref in sums:
        pltpu.matmul_pop(total_ref)

    pl.semaphore_wait(barrier, lines * cols + 1)

    def remote(source, target, send, recv, **where):
        return pltpu.make_async_remote_copy(
            src_ref=source, dst_ref=target, send_sem=send, recv_sem=recv,
            device_id=where, device_id_type=MESH,
        )

    def relay(s, h, j, k):
        ref = xbuf.at[s, h, j, k]
        return remote(ref, ref, pair_send.at[h, j, k], x_recv.at[s % 2, h, j, k], row=z * 2 + 1 - x)

    def routes(s, h, k):
        first = owner * depth
        top = first + depth - 1
        source, target, recv = sbuf.at[s, h, k], xbuf.at[s, h, mine, k], x_recv.at[s % 2, h, mine, k]
        for t in range(lines):
            inside = (t >= first) & (t <= top)
            direct = inside | (jnp.where(t > top, top, first) == z)
            needed = (t != z) & ((own & direct) | (aid & jnp.logical_not(direct)))
            yield needed, remote(source, target, line_send.at[h, t, k], recv, row=t * 2 + x, col=owner)
        yield own, remote(source, target, pair_send.at[h, mine, k], recv, row=z * 2 + 1 - x)

    def spread(s, h, k, again):
        for needed, copy in routes(s, h, k):
            @pl.when(needed)
            def _(copy=copy):
                if again:
                    copy.wait_send()
                copy.start()

    @pl.when(own | aid)
    def _():
        def given(k):
            start = pl.multiple_of((1 - p) * half + k * TILE, TILE)
            return remote(
                v_ref.at[:, pl.ds(start, TILE)], sbuf.at[0, p, k], init_send.at[k], init_recv.at[k], rep=1 - p,
            )

        for k in range(chunks):
            given(k).start()
        for k in range(chunks):
            start = pl.multiple_of(p * half + k * TILE, TILE)
            sbuf[0, p, k] = v_ref[:, pl.ds(start, TILE)]
        @pl.when(p == 0)
        def _():
            for k in range(chunks):
                spread(0, 0, k, False)

        for k in range(chunks):
            given(k).wait()

            @pl.when(p != 0)
            def _(k=k):
                spread(0, 0, k, False)

        for h in range(1, groups):
            for k in range(chunks):
                spread(0, h, k, False)

    @pl.when(own)
    def _():
        for h in range(groups):
            for k in range(chunks):
                run[h, k] = sbuf[0, h, k]
                xbuf[0, h, mine, k] = sbuf[0, h, k]

    @pl.when(jnp.logical_not(own))
    def _():
        run[...] = jnp.zeros_like(run)

    def feed(n, top, rest, large, small):
        pltpu.matmul_push_rhs(large, staging_register=0, mxu_index=n % 2)
        pltpu.matmul_acc_lhs(sums[n], top, load_staged_rhs=0)
        pltpu.matmul_acc_lhs(sums[n], rest)
        pltpu.matmul_push_rhs(small, staging_register=1, mxu_index=n % 2)
        pltpu.matmul_acc_lhs(sums[n], top, load_staged_rhs=1)

    def halves(value):
        top = value.astype(jnp.bfloat16)
        return top, (value - top.astype(jnp.float32)).astype(jnp.bfloat16)

    def prepare(turn, feeding):
        _, _, j, k = chunk_of((turn + middle_step) % total)
        load(turn).wait()
        if feeding:
            top, rest = halves(xbuf[0, 0, j, k])
        for n in range(tiles):
            large, small = halves(stage[turn % SLOTS, n * TILE:(n + 1) * TILE, :])
            large, small = large.T, small.T
            high[j * chunks + k, n] = large
            low[j * chunks + k, n] = small
            if feeding:
                feed(n, top, rest, large, small)

        @pl.when(turn + SLOTS < total)
        def _():
            load(turn + SLOTS).start()

    def pass_on(s, h, place, again):
        _, _, j, k = block_of(0, place)

        @pl.when(r != c * fanout + j)
        def _():
            copy = relay(s, h, j, k)
            copy.wait_recv()
            if again:
                copy.wait_send()
            copy.start()

    def gather(s, h, step, again, ahead):
        if ahead:
            @pl.when(step + AHEAD < total // 2)
            def _():
                pass_on(s, h, step + AHEAD, again)
        else:
            @pl.when(step < total // 2)
            def _():
                pass_on(s, h, step, again)

        _, lane, j, k = chunk_of(step)

        @pl.when(lane != x)
        def _():
            relay(s, h, j, k).wait_recv()

    def multiply(s, h, step):
        _, _, j, k = chunk_of(step)
        index = j * chunks + k
        top, rest = halves(xbuf[s, h, j, k])
        for n in range(tiles):
            feed(n, top, rest, high[index, n], low[index, n])

    def swap(s, h, k):
        return remote(
            acc.at[h, (1 - p) * chunks + k], drecv.at[s, h, k],
            d_send.at[h, k], d_recv.at[s % 2, h, k], rep=1 - p,
        )

    def close(s, h):
        for n in range(tiles):
            acc[h, n] = pltpu.matmul_pop(sums[n])
        for k in range(chunks):
            swap(s, h, k).start()

    def to_column(s, h, k, target):
        ref = ybuf.at[s, h, c, k]
        return remote(ref, ref, y_send.at[target, h, k], y_recv.at[s % 2, c, h, k], col=target)

    def from_column(s, h, k, source):
        ref = ybuf.at[s, h, source, k]
        return remote(ref, ref, y_send.at[source, h, k], y_recv.at[s % 2, source, h, k], col=source)

    def column_sum(s, h, k):
        for offset in range(1, cols):
            from_column(s, h, k, (c + offset) % cols).wait_recv()
        value = ybuf[s, h, 0, k]
        for source in range(1, cols):
            value = value + ybuf[s, h, source, k]
        return value

    def scaled(s, h, k):
        swap(s, h, k).wait_recv()
        degree = jnp.asarray((s + 1) * STEPS, jnp.int32).astype(jnp.float32)
        return (acc[h, p * chunks + k] + drecv[s, h, k]) / degree

    def to_makers(s, h, k, visit):
        for target, there in ((owner, True), (helper, depth > 1)):
            if there:
                @pl.when(c != target)
                def _(target=target):
                    visit(to_column(s, h, k, target))

    def add_up(s, h):
        for k in range(chunks):
            ybuf[s, h, c, k] = scaled(s, h, k)

            @pl.when(s > 0)
            def _(k=k):
                to_makers(s, h, k, lambda copy: copy.wait_send())

            to_makers(s, h, k, lambda copy: copy.start())

    def help_out(s, h):
        @pl.when(aid)
        def _():
            for k in range(chunks):
                sbuf[s + 1, h, k] = column_sum(s, h, k)
                spread(s + 1, h, k, True)

    def send_out(s, h, k):
        @pl.when(own)
        def _():
            value = column_sum(s, h, k)
            sbuf[s + 1, h, k] = value
            spread(s + 1, h, k, True)
            xbuf[s + 1, h, mine, k] = value
            run[h, k] = run[h, k] + value

        swap(s, h, k).wait_send()

    def add_up_last(h):
        for k in range(chunks):
            ybuf[last, h, c, k] = scaled(last, h, k) + run[h, k]

            to_makers(last, h, k, lambda copy: copy.wait_send())
            for offset in range(1, cols):
                to_column(last, h, k, (c + offset) % cols).start()

    def give(k):
        return remote(fin.at[k], frecv.at[k], f_send.at[k], f_recv.at[k], rep=1 - p)

    def finish(h, k):
        value = column_sum(last, h, k)

        @pl.when(p == h)
        def _():
            start = pl.multiple_of(p * half + k * TILE, TILE)
            out_ref[:, pl.ds(start, TILE)] = value

        @pl.when(p != h)
        def _():
            fin[k] = value
            give(k).start()

        swap(last, h, k).wait_send()

    sum_at = jnp.where(p == 0, 0, SUM_AT * total // 16)
    help_at = max(HELP_AT * total // 16, SUM_AT * total // 16)

    def loop(s, h, again, begin, help_on, each, then, start=0):
        def run_step(step, carry):
            if begin is not None:
                @pl.when(step == sum_at)
                def _():
                    begin()

            if help_on is not None:
                @pl.when(step == help_at)
                def _():
                    help_on()

            if each is not None:
                for k in range(chunks):
                    @pl.when(step == total - chunks + k)
                    def _(k=k):
                        each(k)

            gather(s, h, step, again, start == 0)
            if then is not None:
                @pl.when(step >= total - AHEAD)
                def _():
                    pass_on(*then[:2], step - (total - AHEAD), then[2])

            multiply(s, h, step)
            return carry

        lax.fori_loop(start, total, run_step, 0)
        close(s, h)

    def behind(s, h):
        return functools.partial(add_up, s, h), functools.partial(help_out, s, h), functools.partial(send_out, s, h)

    def following(s, h):
        return (s, h + 1, True) if h < groups - 1 else (s + 1, 0, True)

    def split(turn, carry):
        prepare(turn, False)
        return carry

    def split_and_feed(turn, carry):
        gather(0, 0, turn + middle_step - total, False, False)
        prepare(turn, True)
        return carry

    lax.fori_loop(0, total - middle_step, split, 0)
    lax.fori_loop(total - middle_step, total, split_and_feed, 0)
    loop(0, 0, False, None, None, None, (0, 1, False), middle_step)
    for h in range(1, groups):
        loop(0, h, False, *behind(0, h - 1), following(0, h))

    def middle(s, carry):
        loop(s, 0, True, *behind(s - 1, groups - 1), following(s, 0))
        for h in range(1, groups):
            loop(s, h, True, *behind(s, h - 1), following(s, h))
        return carry

    lax.fori_loop(1, last, middle, 0)
    loop(last, 0, True, *behind(last - 1, groups - 1), following(last, 0))
    for h in range(1, groups):
        loop(last, h, True, functools.partial(add_up_last, h - 1), None, functools.partial(finish, h - 1),
             following(last, h) if h < groups - 1 else None)
    add_up_last(groups - 1)
    for k in range(chunks):
        finish(groups - 1, k)

    for k in range(chunks):
        give(k).wait()
        start = pl.multiple_of((1 - p) * half + k * TILE, TILE)
        out_ref[:, pl.ds(start, TILE)] = frecv[k]
        for h in range(groups):
            for offset in range(1, cols):
                to_column(last, h, k, (c + offset) % cols).wait_send()

    def drain(step, carry):
        _, lane, j, k = chunk_of(step)

        @pl.when(lane == x)
        def _():
            for h in range(groups):
                relay(last, h, j, k).wait_send()

        return carry

    lax.fori_loop(0, total, drain, 0)
    for h in range(groups):
        for k in range(chunks):
            for needed, copy in list(routes(last, h, k))[:-1]:
                @pl.when(needed)
                def _(copy=copy):
                    copy.wait_send()


def solution(mesh):
    rows, cols, groups = (mesh.shape[axis] for axis in ("row", "col", "rep"))

    def local(matrix, vectors):
        size, width = matrix.shape
        part = vectors.shape[0]
        fanout = rows // cols
        chunks = size // 2 // TILE
        tiles = size // TILE
        piece = (part, TILE)
        dma = pltpu.SemaphoreType.DMA
        return pl.pallas_call(
            functools.partial(kernel, rows, cols, groups),
            out_shape=jax.ShapeDtypeStruct(vectors.shape, jnp.float32),
            in_specs=[pl.BlockSpec(memory_space=pltpu.HBM), pl.BlockSpec(memory_space=pltpu.VMEM)],
            out_specs=pl.BlockSpec(memory_space=pltpu.VMEM),
            scratch_shapes=[
                pltpu.VMEM((fanout * chunks, tiles, TILE, TILE), jnp.bfloat16),
                pltpu.VMEM((fanout * chunks, tiles, TILE, TILE), jnp.bfloat16),
                pltpu.VMEM((SLOTS, size, TILE), jnp.float32),
                pltpu.VMEM((TERMS, groups, fanout, chunks) + piece, jnp.float32),
                pltpu.VMEM((TERMS, groups, chunks) + piece, jnp.float32),
                pltpu.VMEM((groups, tiles) + piece, jnp.float32),
                pltpu.VMEM((TERMS, groups, chunks) + piece, jnp.float32),
                pltpu.VMEM((TERMS, groups, cols, chunks) + piece, jnp.float32),
                pltpu.VMEM((groups, chunks) + piece, jnp.float32),
                pltpu.VMEM((chunks,) + piece, jnp.float32),
                pltpu.VMEM((chunks,) + piece, jnp.float32),
                dma((SLOTS,)),
                dma((chunks,)),
                dma((chunks,)),
                dma((2, groups, fanout, chunks)),
                dma((groups, rows // 2, chunks)),
                dma((groups, fanout, chunks)),
                dma((groups, chunks)),
                dma((2, groups, chunks)),
                dma((cols, groups, chunks)),
                dma((2, cols, groups, chunks)),
                dma((chunks,)),
                dma((chunks,)),
            ],
            compiler_params=pltpu.CompilerParams(
                collective_id=0, has_side_effects=True, vmem_limit_bytes=63 * 1024 * 1024
            ),
        )(matrix, vectors)

    return jax.shard_map(
        local, mesh=mesh, in_specs=(P("row", "col"), P("rep", "row")), out_specs=P("rep", "row"), check_vma=False
    )
```

```python
import functools

import jax
import jax.numpy as jnp
from jax import lax
from jax.experimental import pallas as pl
from jax.experimental.pallas import tpu as pltpu
from jax.sharding import PartitionSpec as P

TERMS = 6
STEPS = 1
MESH = pl.DeviceIdType.MESH
TILE = 256
SLOTS = 4
LAG = 5
SUM_AT = 3
HELP_AT = 5
AHEAD = 1


def kernel(rows, cols, groups, *refs):
    tiles = refs[0].shape[0] // TILE
    part = refs[1].shape[0]
    sums = [pltpu.ACC(n % 2)((part, TILE), jnp.float32) for n in range(tiles)]
    pl.run_scoped(lambda *sums: body(rows, cols, groups, sums, *refs), *sums)


def body(
    rows, cols, groups, sums, m_ref, v_ref, out_ref,
    high, low, stage, xbuf, sbuf, acc, drecv, ybuf, run, fin, frecv,
    stage_sem, init_send, init_recv, x_recv, line_send, pair_send,
    d_send, d_recv, y_send, y_recv, f_send, f_recv,
):
    fanout = rows // cols
    size = m_ref.shape[0]
    part = v_ref.shape[0]
    half = size // 2
    chunks = half // TILE
    tiles = size // TILE
    lines = rows // 2
    depth = fanout // 2
    total = fanout * chunks
    last = TERMS - 1

    r, c, p = lax.axis_index("row"), lax.axis_index("col"), lax.axis_index("rep")
    z, x = r // 2, r % 2
    first_line = c * depth
    owner = r // fanout
    own = owner == c
    helper = (owner + 1) % cols
    aid = (helper == c) & (depth > 1)
    mine = r % fanout

    barrier = pltpu.get_barrier_semaphore()

    def greet(**where):
        pl.semaphore_signal(barrier, inc=1, device_id=where, device_id_type=MESH)

    greet(rep=1 - p)
    greet(row=z * 2 + 1 - x)
    for other in range(1, lines * cols):
        greet(row=(z + other // cols) % lines * 2 + x, col=(c + other % cols) % cols)

    def chunk_of(step):
        count = total // 2
        lag = min(LAG, count)
        mixed = step - lag
        alternate = jnp.where(mixed % 2 == 0, count + mixed // 2, lag + mixed // 2)
        place = jnp.where(step < lag, step, jnp.where(step < 2 * count - lag, alternate, step))
        return block_of(place // count, place % count)

    def block_of(other, place):
        near = jnp.where(own, place // chunks, place % depth)
        line = jnp.where(z > first_line, depth - 1 - near, near)
        lane = jnp.where(other == 0, x, 1 - x)
        return line, lane, line * 2 + lane, jnp.where(own, place % chunks, place // depth)

    middle_step = total // 2

    def load(turn):
        _, _, j, k = chunk_of((turn + middle_step) % total)
        start = pl.multiple_of(j * size + p * half + k * TILE, TILE)
        return pltpu.make_async_copy(
            m_ref.at[:, pl.ds(start, TILE)], stage.at[turn % SLOTS], stage_sem.at[turn % SLOTS]
        )

    for step in range(min(SLOTS, total)):
        load(step).start()

    for total_ref in sums:
        pltpu.matmul_pop(total_ref)

    pl.semaphore_wait(barrier, lines * cols + 1)

    def remote(source, target, send, recv, **where):
        return pltpu.make_async_remote_copy(
            src_ref=source, dst_ref=target, send_sem=send, recv_sem=recv,
            device_id=where, device_id_type=MESH,
        )

    def relay(s, h, j, k):
        ref = xbuf.at[s, h, j, k]
        return remote(ref, ref, pair_send.at[h, j, k], x_recv.at[s % 2, h, j, k], row=z * 2 + 1 - x)

    def routes(s, h, k):
        first = owner * depth
        top = first + depth - 1
        source, target, recv = sbuf.at[s, h, k], xbuf.at[s, h, mine, k], x_recv.at[s % 2, h, mine, k]
        for t in range(lines):
            inside = (t >= first) & (t <= top)
            direct = inside | (jnp.where(t > top, top, first) == z)
            needed = (t != z) & ((own & direct) | (aid & jnp.logical_not(direct)))
            yield needed, remote(source, target, line_send.at[h, t, k], recv, row=t * 2 + x, col=owner)
        yield own, remote(source, target, pair_send.at[h, mine, k], recv, row=z * 2 + 1 - x)

    def spread(s, h, k, again):
        for needed, copy in routes(s, h, k):
            @pl.when(needed)
            def _(copy=copy):
                if again:
                    copy.wait_send()
                copy.start()

    @pl.when(own | aid)
    def _():
        def given(k):
            start = pl.multiple_of((1 - p) * half + k * TILE, TILE)
            return remote(
                v_ref.at[:, pl.ds(start, TILE)], sbuf.at[0, p, k], init_send.at[k], init_recv.at[k], rep=1 - p,
            )

        for k in range(chunks):
            given(k).start()
        for k in range(chunks):
            start = pl.multiple_of(p * half + k * TILE, TILE)
            sbuf[0, p, k] = v_ref[:, pl.ds(start, TILE)]
        @pl.when(p == 0)
        def _():
            for k in range(chunks):
                spread(0, 0, k, False)

        for k in range(chunks):
            given(k).wait()

            @pl.when(p != 0)
            def _(k=k):
                spread(0, 0, k, False)

        for h in range(1, groups):
            for k in range(chunks):
                spread(0, h, k, False)

    @pl.when(own)
    def _():
        for h in range(groups):
            for k in range(chunks):
                run[h, k] = sbuf[0, h, k]
                xbuf[0, h, mine, k] = sbuf[0, h, k]

    @pl.when(jnp.logical_not(own))
    def _():
        run[...] = jnp.zeros_like(run)

    def feed(n, top, rest, large, small):
        pltpu.matmul_push_rhs(large, staging_register=0, mxu_index=n % 2)
        pltpu.matmul_acc_lhs(sums[n], top, load_staged_rhs=0)
        pltpu.matmul_acc_lhs(sums[n], rest)
        pltpu.matmul_push_rhs(small, staging_register=1, mxu_index=n % 2)
        pltpu.matmul_acc_lhs(sums[n], top, load_staged_rhs=1)

    def halves(value):
        top = value.astype(jnp.bfloat16)
        return top, (value - top.astype(jnp.float32)).astype(jnp.bfloat16)

    def prepare(turn, feeding):
        _, _, j, k = chunk_of((turn + middle_step) % total)
        load(turn).wait()
        if feeding:
            top, rest = halves(xbuf[0, 0, j, k])
        for n in range(tiles):
            large, small = halves(stage[turn % SLOTS, n * TILE:(n + 1) * TILE, :])
            large, small = large.T, small.T
            high[j * chunks + k, n] = large
            low[j * chunks + k, n] = small
            if feeding:
                feed(n, top, rest, large, small)

        @pl.when(turn + SLOTS < total)
        def _():
            load(turn + SLOTS).start()

    def pass_on(s, h, place, again):
        _, _, j, k = block_of(0, place)

        @pl.when(r != c * fanout + j)
        def _():
            copy = relay(s, h, j, k)
            copy.wait_recv()
            if again:
                copy.wait_send()
            copy.start()

    def gather(s, h, step, again, ahead):
        if ahead:
            @pl.when(step + AHEAD < total // 2)
            def _():
                pass_on(s, h, step + AHEAD, again)
        else:
            @pl.when(step < total // 2)
            def _():
                pass_on(s, h, step, again)

        _, lane, j, k = chunk_of(step)

        @pl.when(lane != x)
        def _():
            relay(s, h, j, k).wait_recv()

    def multiply(s, h, step):
        _, _, j, k = chunk_of(step)
        index = j * chunks + k
        top, rest = halves(xbuf[s, h, j, k])
        for n in range(tiles):
            feed(n, top, rest, high[index, n], low[index, n])

    def swap(s, h, k):
        return remote(
            acc.at[h, (1 - p) * chunks + k], drecv.at[s, h, k],
            d_send.at[h, k], d_recv.at[s % 2, h, k], rep=1 - p,
        )

    def close(s, h):
        for n in range(tiles):
            acc[h, n] = pltpu.matmul_pop(sums[n])
        for k in range(chunks):
            swap(s, h, k).start()

    def to_column(s, h, k, target):
        ref = ybuf.at[s, h, c, k]
        return remote(ref, ref, y_send.at[target, h, k], y_recv.at[s % 2, c, h, k], col=target)

    def from_column(s, h, k, source):
        ref = ybuf.at[s, h, source, k]
        return remote(ref, ref, y_send.at[source, h, k], y_recv.at[s % 2, source, h, k], col=source)

    def column_sum(s, h, k):
        for offset in range(1, cols):
            from_column(s, h, k, (c + offset) % cols).wait_recv()
        value = ybuf[s, h, 0, k]
        for source in range(1, cols):
            value = value + ybuf[s, h, source, k]
        return value

    def scaled(s, h, k):
        swap(s, h, k).wait_recv()
        degree = jnp.asarray((s + 1) * STEPS, jnp.int32).astype(jnp.float32)
        return (acc[h, p * chunks + k] + drecv[s, h, k]) / degree

    def to_makers(s, h, k, visit):
        for target, there in ((owner, True), (helper, depth > 1)):
            if there:
                @pl.when(c != target)
                def _(target=target):
                    visit(to_column(s, h, k, target))

    def add_up(s, h):
        for k in range(chunks):
            ybuf[s, h, c, k] = scaled(s, h, k)

            @pl.when(s > 0)
            def _(k=k):
                to_makers(s, h, k, lambda copy: copy.wait_send())

            to_makers(s, h, k, lambda copy: copy.start())

    def help_out(s, h, k):
        @pl.when(aid)
        def _():
            sbuf[s + 1, h, k] = column_sum(s, h, k)
            spread(s + 1, h, k, True)

    def send_out(s, h, k):
        @pl.when(own)
        def _():
            value = column_sum(s, h, k)
            sbuf[s + 1, h, k] = value
            spread(s + 1, h, k, True)
            xbuf[s + 1, h, mine, k] = value
            run[h, k] = run[h, k] + value

        swap(s, h, k).wait_send()

    def add_up_last(h):
        for k in range(chunks):
            ybuf[last, h, c, k] = scaled(last, h, k) + run[h, k]

            to_makers(last, h, k, lambda copy: copy.wait_send())
            for offset in range(1, cols):
                to_column(last, h, k, (c + offset) % cols).start()

    def give(k):
        return remote(fin.at[k], frecv.at[k], f_send.at[k], f_recv.at[k], rep=1 - p)

    def finish(h, k):
        value = column_sum(last, h, k)

        @pl.when(p == h)
        def _():
            start = pl.multiple_of(p * half + k * TILE, TILE)
            out_ref[:, pl.ds(start, TILE)] = value

        @pl.when(p != h)
        def _():
            fin[k] = value
            give(k).start()

        swap(last, h, k).wait_send()

    sum_at = jnp.where(p == 0, 1, SUM_AT) * total // 16
    help_at = max(HELP_AT * total // 16, SUM_AT * total // 16)

    def loop(s, h, again, begin, help_on, each, then, start=0):
        def run_step(step, carry):
            if begin is not None:
                @pl.when(step == sum_at)
                def _():
                    begin()

            if help_on is not None:
                for k in range(chunks):
                    @pl.when(step == min(help_at + k, total - 1))
                    def _(k=k):
                        help_on(k)

            if each is not None:
                for k in range(chunks):
                    @pl.when(step == total - chunks + k)
                    def _(k=k):
                        each(k)

            gather(s, h, step, again, start == 0)
            if then is not None:
                @pl.when(step >= total - AHEAD)
                def _():
                    pass_on(*then[:2], step - (total - AHEAD), then[2])

            multiply(s, h, step)
            return carry

        lax.fori_loop(start, total, run_step, 0)
        close(s, h)

    def behind(s, h):
        return functools.partial(add_up, s, h), functools.partial(help_out, s, h), functools.partial(send_out, s, h)

    def following(s, h):
        return (s, h + 1, True) if h < groups - 1 else (s + 1, 0, True)

    def split(turn, carry):
        prepare(turn, False)
        return carry

    def split_and_feed(turn, carry):
        gather(0, 0, turn + middle_step - total, False, False)
        prepare(turn, True)
        return carry

    lax.fori_loop(0, total - middle_step, split, 0)
    lax.fori_loop(total - middle_step, total, split_and_feed, 0)
    loop(0, 0, False, None, None, None, (0, 1, False), middle_step)
    for h in range(1, groups):
        loop(0, h, False, *behind(0, h - 1), following(0, h))

    def middle(s, carry):
        loop(s, 0, True, *behind(s - 1, groups - 1), following(s, 0))
        for h in range(1, groups):
            loop(s, h, True, *behind(s, h - 1), following(s, h))
        return carry

    lax.fori_loop(1, last, middle, 0)
    loop(last, 0, True, *behind(last - 1, groups - 1), following(last, 0))
    for h in range(1, groups):
        loop(last, h, True, functools.partial(add_up_last, h - 1), None, functools.partial(finish, h - 1),
             following(last, h) if h < groups - 1 else None)
    add_up_last(groups - 1)
    for k in range(chunks):
        finish(groups - 1, k)

    for k in range(chunks):
        give(k).wait()
        start = pl.multiple_of((1 - p) * half + k * TILE, TILE)
        out_ref[:, pl.ds(start, TILE)] = frecv[k]
        for h in range(groups):
            for offset in range(1, cols):
                to_column(last, h, k, (c + offset) % cols).wait_send()

    def drain(step, carry):
        _, lane, j, k = chunk_of(step)

        @pl.when(lane == x)
        def _():
            for h in range(groups):
                relay(last, h, j, k).wait_send()

        return carry

    lax.fori_loop(0, total, drain, 0)
    for h in range(groups):
        for k in range(chunks):
            for needed, copy in list(routes(last, h, k))[:-1]:
                @pl.when(needed)
                def _(copy=copy):
                    copy.wait_send()


def solution(mesh):
    rows, cols, groups = (mesh.shape[axis] for axis in ("row", "col", "rep"))

    def local(matrix, vectors):
        size, width = matrix.shape
        part = vectors.shape[0]
        fanout = rows // cols
        chunks = size // 2 // TILE
        tiles = size // TILE
        piece = (part, TILE)
        dma = pltpu.SemaphoreType.DMA
        return pl.pallas_call(
            functools.partial(kernel, rows, cols, groups),
            out_shape=jax.ShapeDtypeStruct(vectors.shape, jnp.float32),
            in_specs=[pl.BlockSpec(memory_space=pltpu.HBM), pl.BlockSpec(memory_space=pltpu.VMEM)],
            out_specs=pl.BlockSpec(memory_space=pltpu.VMEM),
            scratch_shapes=[
                pltpu.VMEM((fanout * chunks, tiles, TILE, TILE), jnp.bfloat16),
                pltpu.VMEM((fanout * chunks, tiles, TILE, TILE), jnp.bfloat16),
                pltpu.VMEM((SLOTS, size, TILE), jnp.float32),
                pltpu.VMEM((TERMS, groups, fanout, chunks) + piece, jnp.float32),
                pltpu.VMEM((TERMS, groups, chunks) + piece, jnp.float32),
                pltpu.VMEM((groups, tiles) + piece, jnp.float32),
                pltpu.VMEM((TERMS, groups, chunks) + piece, jnp.float32),
                pltpu.VMEM((TERMS, groups, cols, chunks) + piece, jnp.float32),
                pltpu.VMEM((groups, chunks) + piece, jnp.float32),
                pltpu.VMEM((chunks,) + piece, jnp.float32),
                pltpu.VMEM((chunks,) + piece, jnp.float32),
                dma((SLOTS,)),
                dma((chunks,)),
                dma((chunks,)),
                dma((2, groups, fanout, chunks)),
                dma((groups, rows // 2, chunks)),
                dma((groups, fanout, chunks)),
                dma((groups, chunks)),
                dma((2, groups, chunks)),
                dma((cols, groups, chunks)),
                dma((2, cols, groups, chunks)),
                dma((chunks,)),
                dma((chunks,)),
            ],
            compiler_params=pltpu.CompilerParams(
                collective_id=0, has_side_effects=True, vmem_limit_bytes=63 * 1024 * 1024
            ),
        )(matrix, vectors)

    return jax.shard_map(
        local, mesh=mesh, in_specs=(P("row", "col"), P("rep", "row")), out_specs=P("rep", "row"), check_vma=False
    )
```
